32 devices in a mesh: dp: 1 (over z), tp: 32 (over y, x, core).
Axes of the slice: x: 4, y: 4, z: 1, core: 2. Of those that a mesh axis runs over, the one named last changes fastest.
The devices are a block of a 4x4x8 slice.
Arguments:
- hidden: bfloat16 [4096, 2048], P(('dp', 'tp'))
- w_head: bfloat16 [2048, 128256], P(None, 'tp')
- labels: int32 [4096], P(('dp', 'tp'))
Outputs:
- output 1: float32 [1], P('dp')
- output 2: bfloat16 [4096, 2048], P(('dp', 'tp'))
- output 3: bfloat16 [2048, 128256], P('dp', 'tp')
All inputs are finite; a program needn't handle non-finite values.
Results may differ from the reference program's by a relative error of at most 0.001.
Values are sent between devices in bfloat16 or wider.
A program may use at most 768 MiB of HBM per device.

```python
import math
import jax
import jax.numpy as jnp
from jax import lax

HIDDEN = 2048
VOCAB = 128256
TOKENS = 4096

ROW_BLOCK = math.gcd(TOKENS, 64)


def setup_inputs(seed: int = 0, part: int = 0) -> dict:
    base_key = jax.random.key(seed)
    key_w, key_parts = jax.random.split(base_key)
    key_x, key_lab = jax.random.split(jax.random.fold_in(key_parts, part))
    w_head = jax.random.normal(key_w, (HIDDEN, VOCAB), jnp.float32) * HIDDEN ** -0.5
    labels = jax.random.randint(key_lab, (TOKENS,), 0, VOCAB, dtype=jnp.int32)
    label_boost = math.log(VOCAB) - 1.0
    noise_x = jax.random.normal(key_x, (TOKENS, HIDDEN), jnp.float32)
    hidden = noise_x + label_boost * jnp.take(w_head, labels, axis=1).T
    return {"hidden": hidden.astype(jnp.bfloat16), "w_head": w_head.astype(jnp.bfloat16), "labels": labels}


def reference(hidden, w_head, labels):
    inv_tokens = 1.0 / TOKENS
    num_blocks = TOKENS // ROW_BLOCK
    hid_blocks = hidden.reshape(num_blocks, ROW_BLOCK, HIDDEN)
    lab_blocks = labels.reshape(num_blocks, ROW_BLOCK)
    vocab_ids = jnp.arange(VOCAB, dtype=jnp.int32)
    w_trans = w_head.T

    def row_step(acc_dw, block):
        hid_blk, lab_blk = block
        logits = jnp.dot(hid_blk, w_head, preferred_element_type=jnp.float32)
        row_max = jnp.max(logits, axis=1, keepdims=True)
        shifted = jnp.exp(logits - row_max)
        row_sum = jnp.sum(shifted, axis=1, keepdims=True)
        onehot = (vocab_ids[None, :] == lab_blk[:, None]).astype(jnp.float32)
        target = jnp.sum(logits * onehot, axis=1)
        token_loss = row_max[:, 0] + jnp.log(row_sum[:, 0]) - target
        grad_out = ((shifted / row_sum - onehot) * inv_tokens).astype(jnp.bfloat16)
        acc_dw = acc_dw + jnp.dot(hid_blk.T, grad_out, preferred_element_type=jnp.float32)
        dx_blk = jnp.dot(grad_out, w_trans, preferred_element_type=jnp.float32)
        return acc_dw, (token_loss, dx_blk.astype(jnp.bfloat16))

    zero_dw = jnp.zeros((HIDDEN, VOCAB), jnp.float32)
    acc_dw, (losses, dx_blocks) = lax.scan(row_step, zero_dw, (hid_blocks, lab_blocks))
    mean_loss = (jnp.sum(losses) * inv_tokens).reshape(1)
    return mean_loss, dx_blocks.reshape(TOKENS, HIDDEN), acc_dw.astype(jnp.bfloat16)
```

```python
import functools
import math

import jax
import jax.numpy as jnp
from jax import lax
from jax.experimental import pallas as pl
from jax.experimental.pallas import tpu as pltpu
from jax.sharding import PartitionSpec as P

MESH = pl.DeviceIdType.MESH
LANES = 128
TT = 512
CT = 512
NEG = -3.0e38
VMEM_LIMIT = 60 * 1024 * 1024


def share_kernel(n, x_ref, out_ref, send_sem, recv_sem):
    me = lax.axis_index("tp")
    barrier = pltpu.get_barrier_semaphore()

    def greet(k, carry):
        pl.semaphore_signal(barrier, inc=1, device_id={"tp": lax.rem(me + k, n)}, device_id_type=MESH)
        return carry

    lax.fori_loop(1, n, greet, 0)
    pl.semaphore_wait(barrier, n - 1)

    def copy_to(k):
        peer = lax.rem(me + k, n)
        return pltpu.make_async_remote_copy(
            src_ref=x_ref,
            dst_ref=out_ref.at[me],
            send_sem=send_sem.at[peer],
            recv_sem=recv_sem.at[me],
            device_id={"tp": peer},
            device_id_type=MESH,
        )

    def start(k, carry):
        copy_to(k).start()
        return carry

    lax.fori_loop(1, n, start, 0)
    out_ref[me] = x_ref[...]

    def finish(k, carry):
        peer = lax.rem(me + k, n)
        copy_to(k).wait_send()
        pltpu.make_async_remote_copy(
            src_ref=x_ref,
            dst_ref=out_ref.at[peer],
            send_sem=send_sem.at[peer],
            recv_sem=recv_sem.at[peer],
            device_id={"tp": peer},
            device_id_type=MESH,
        ).wait_recv()
        return carry

    lax.fori_loop(1, n, finish, 0)


def share(x, n, ident):
    return pl.pallas_call(
        functools.partial(share_kernel, n),
        name=f"share{ident}",
        out_shape=jax.ShapeDtypeStruct((n, *x.shape), x.dtype),
        in_specs=[pl.BlockSpec(memory_space=pltpu.VMEM)],
        out_specs=pl.BlockSpec(memory_space=pltpu.VMEM),
        scratch_shapes=[pltpu.SemaphoreType.DMA((n,)), pltpu.SemaphoreType.DMA((n,))],
        compiler_params=pltpu.CompilerParams(collective_id=ident, has_side_effects=True),
    )(x)


def load_head(w_hbm, w_tail, w_scr, sem, start):
    width = w_scr.shape[1] - LANES
    a = pltpu.make_async_copy(w_hbm.at[:, pl.ds(0, width)], w_scr.at[:, pl.ds(0, width)], sem.at[0])
    b = pltpu.make_async_copy(w_tail, w_scr.at[:, pl.ds(width, LANES)], sem.at[1])
    for c in (a, b):
        if start:
            c.start()
        else:
            c.wait()


def fwd_kernel(vocab, x_ref, w_hbm, w_tail, z_ref, xt_ref, m_ref, s_ref, w_scr, zb0, zb1, sem):
    padded = w_scr.shape[1]
    tiles = padded // CT
    depth = x_ref.shape[1] // tiles

    @pl.when(pl.program_id(0) == 0)
    def _():
        load_head(w_hbm, w_tail, w_scr, sem, True)
        load_head(w_hbm, w_tail, w_scr, sem, False)

    m_ref[...] = jnp.full(m_ref.shape, NEG, jnp.float32)
    s_ref[...] = jnp.zeros(s_ref.shape, jnp.float32)
    lane = lax.broadcasted_iota(jnp.int32, (32, LANES), 1)

    def product(j, zb):
        zb[...] = jnp.dot(
            x_ref[...], w_scr[:, pl.ds(pl.multiple_of(j * CT, CT), CT)], preferred_element_type=jnp.float32
        )
        at = pl.ds(pl.multiple_of(j * depth, depth), depth)
        xt_ref[at, :] = x_ref[:, at].T

    def absorb(j, zb):
        last = CT // LANES - 1
        room = vocab - j * CT - last * LANES
        for r in range(0, TT, 32):
            rows = pl.ds(r, 32)
            zs = [zb[rows, pl.ds(k * LANES, LANES)] for k in range(CT // LANES)]
            for k in range(CT // LANES):
                z_ref[rows, pl.ds(pl.multiple_of(j * CT + k * LANES, LANES), LANES)] = zs[k]
            zs[last] = jnp.where(lane < room, zs[last], NEG)
            m_old = m_ref[rows, :]
            m_new = m_old
            for z in zs:
                m_new = jnp.maximum(m_new, z)
            total = s_ref[rows, :] * jnp.exp(m_old - m_new)
            for z in zs:
                total = total + jnp.exp(z - m_new)
            m_ref[rows, :] = m_new
            s_ref[rows, :] = total

    product(0, zb0)

    def pair(p, carry):
        product(2 * p + 1, zb1)
        absorb(2 * p, zb0)
        product(2 * p + 2, zb0)
        absorb(2 * p + 1, zb1)
        return carry

    lax.fori_loop(0, tiles // 2 - 1, pair, 0)
    product(tiles - 1, zb1)
    absorb(tiles - 2, zb0)
    absorb(tiles - 1, zb1)


def forward(x, w, w_tail):
    tokens, hidden = x.shape
    padded = w.shape[1] // LANES * LANES + LANES
    any_spec = pl.BlockSpec(memory_space=pl.ANY)
    return pl.pallas_call(
        functools.partial(fwd_kernel, w.shape[1]),
        name="forward",
        grid=(tokens // TT,),
        out_shape=(
            jax.ShapeDtypeStruct((tokens, padded), jnp.float32),
            jax.ShapeDtypeStruct((hidden, tokens), jnp.bfloat16),
            jax.ShapeDtypeStruct((tokens, LANES), jnp.float32),
            jax.ShapeDtypeStruct((tokens, LANES), jnp.float32),
        ),
        in_specs=[pl.BlockSpec((TT, hidden), lambda i: (i, 0)), any_spec, any_spec],
        out_specs=(
            pl.BlockSpec((TT, padded), lambda i: (i, 0)),
            pl.BlockSpec((hidden, TT), lambda i: (0, i)),
            pl.BlockSpec((TT, LANES), lambda i: (i, 0)),
            pl.BlockSpec((TT, LANES), lambda i: (i, 0)),
        ),
        scratch_shapes=[
            pltpu.VMEM((hidden, padded), jnp.bfloat16),
            pltpu.VMEM((TT, CT), jnp.float32),
            pltpu.VMEM((TT, CT), jnp.float32),
            pltpu.SemaphoreType.DMA((2,)),
        ],
        compiler_params=pltpu.CompilerParams(vmem_limit_bytes=VMEM_LIMIT),
        cost_estimate=pl.CostEstimate(flops=2 * tokens * hidden * padded, bytes_accessed=6 * tokens * padded, transcendentals=0),
    )(x, w, w_tail)


def grad_kernel(inv, z_ref, lse_ref, lab_ref, w_hbm, w_tail, g_ref, dx_ref, t_ref, w_scr, g0, g1, sem):
    padded = w_scr.shape[1]
    hidden = w_scr.shape[0]
    step = pl.program_id(0)
    steps = pl.num_programs(0)
    pieces = padded // CT
    width = hidden // pieces
    lane = lax.broadcasted_iota(jnp.int32, (32, LANES), 1)

    def probs(j, g):
        for r in range(0, TT, 32):
            rows = pl.ds(r, 32)
            lse = lse_ref[rows, :]
            rel = lab_ref[rows, :] - j * CT
            t = t_ref[...]
            for k in range(CT // LANES):
                at = pl.ds(pl.multiple_of(j * CT + k * LANES, LANES), LANES)
                z = z_ref[rows, at]
                p = jnp.exp(z - lse)
                hit = rel == lane + k * LANES
                t = t + jnp.where(hit, z, 0.0)
                gv = jnp.where(hit, p - inv, p).astype(jnp.bfloat16)
                g[rows, at] = gv
                g_ref[rows, at] = gv
            t_ref[...] = t

    @pl.when(step == 0)
    def _():
        load_head(w_hbm, w_tail, w_scr, sem, True)
        t_ref[...] = jnp.zeros(t_ref.shape, jnp.float32)

        def piece(j, carry):
            probs(j, g0)
            return carry

        lax.fori_loop(0, pieces, piece, 0)
        load_head(w_hbm, w_tail, w_scr, sem, False)

    def back(j, g):
        at = pl.ds(pl.multiple_of(j * width, width), width)
        dx_ref[:, at] = lax.dot_general(
            g[...], w_scr[at, :], (((1,), (1,)), ((), ())), preferred_element_type=jnp.float32
        )

    for parity, (now, later) in enumerate(((g1, g0), (g0, g1))):

        @pl.when((step > 0) & (step < steps - 1) & (lax.rem(step, 2) == parity))
        def _(now=now, later=later):
            def piece(j, carry):
                back(j, now)
                probs(j, later)
                return carry

            lax.fori_loop(0, pieces, piece, 0)

    @pl.when(step == steps - 1)
    def _():
        def piece(j, carry):
            back(j, g1)
            return carry

        lax.fori_loop(0, pieces, piece, 0)


def grad_rows(z, lse, lab, w, w_tail, inv):
    tokens, padded = z.shape
    hidden = w.shape[0]
    steps = tokens // TT
    any_spec = pl.BlockSpec(memory_space=pl.ANY)
    ahead = lambda i: (jnp.minimum(i, steps - 1), 0)
    return pl.pallas_call(
        functools.partial(grad_kernel, inv),
        name="grad_rows",
        grid=(steps + 1,),
        out_shape=(
            jax.ShapeDtypeStruct((tokens, padded), jnp.bfloat16),
            jax.ShapeDtypeStruct((tokens, hidden), jnp.float32),
            jax.ShapeDtypeStruct((32, LANES), jnp.float32),
        ),
        in_specs=[
            pl.BlockSpec((TT, padded), ahead),
            pl.BlockSpec((TT, LANES), ahead),
            pl.BlockSpec((TT, LANES), ahead),
            any_spec,
            any_spec,
        ],
        out_specs=(
            pl.BlockSpec((TT, padded), ahead),
            pl.BlockSpec((TT, hidden), lambda i: (jnp.maximum(i - 1, 0), 0)),
            pl.BlockSpec((32, LANES), lambda i: (0, 0)),
        ),
        scratch_shapes=[
            pltpu.VMEM((hidden, padded), jnp.bfloat16),
            pltpu.VMEM((TT, padded), jnp.bfloat16),
            pltpu.VMEM((TT, padded), jnp.bfloat16),
            pltpu.SemaphoreType.DMA((2,)),
        ],
        compiler_params=pltpu.CompilerParams(vmem_limit_bytes=VMEM_LIMIT),
        cost_estimate=pl.CostEstimate(flops=2 * tokens * hidden * padded, bytes_accessed=6 * tokens * padded, transcendentals=0),
    )(z, lse, lab, w, w_tail)


def head_kernel(xt_ref, g_ref, out_ref):
    def piece(j, carry):
        rows = pl.ds(pl.multiple_of(j * TT, TT), TT)
        out_ref[rows, :] = jnp.dot(xt_ref[rows, :], g_ref[...], preferred_element_type=jnp.float32).astype(jnp.bfloat16)
        return carry

    lax.fori_loop(0, xt_ref.shape[0] // TT, piece, 0)


def grad_head(xt, g, vocab):
    hidden, tokens = xt.shape
    padded = g.shape[1]
    width = 256
    return pl.pallas_call(
        head_kernel,
        name="grad_head",
        grid=(padded // width,),
        out_shape=jax.ShapeDtypeStruct((hidden, vocab), jnp.bfloat16),
        in_specs=[
            pl.BlockSpec((hidden, tokens), lambda i: (0, 0), pipeline_mode=pl.Buffered(1)),
            pl.BlockSpec((tokens, width), lambda i: (0, i)),
        ],
        out_specs=pl.BlockSpec((hidden, width), lambda i: (0, i)),
        compiler_params=pltpu.CompilerParams(vmem_limit_bytes=VMEM_LIMIT),
        cost_estimate=pl.CostEstimate(flops=2 * tokens * hidden * padded, bytes_accessed=4 * tokens * padded, transcendentals=0),
    )(xt, g)


def solution(mesh):
    n = mesh.shape["tp"]

    def local_step(hid_loc, w_loc, lab_loc):
        rows, hidden = hid_loc.shape
        vocab = w_loc.shape[1]
        tokens = rows * n
        inv = 1.0 / tokens
        even = vocab // LANES * LANES
        w_tail = jnp.pad(w_loc[:, even:], ((0, 0), (0, even + LANES - vocab)))
        lab_all = share(jnp.broadcast_to(lab_loc.reshape(1, rows), (8, rows)), n, 0)[:, 0, :]
        hid_all = lax.all_gather(hid_loc, "tp", axis=0, tiled=True)
        z, xt, m_lane, s_lane = forward(hid_all, w_loc, w_tail)
        m_loc = jnp.max(m_lane, axis=1)
        s_loc = jnp.sum(s_lane * jnp.exp(m_lane - m_loc[:, None]), axis=1)
        stats = share(jnp.concatenate([m_loc.reshape(-1, LANES), s_loc.reshape(-1, LANES)]), n, 1)
        m_all, s_all = stats[:, : tokens // LANES], stats[:, tokens // LANES :]
        m_glob = jnp.max(m_all, axis=0)
        s_glob = jnp.sum(s_all * jnp.exp(m_all - m_glob), axis=0)
        lse = m_glob + jnp.log(s_glob)
        lse_b = jnp.broadcast_to((lse + math.log(tokens)).reshape(tokens, 1), (tokens, LANES))
        lab_b = jnp.broadcast_to((lab_all.reshape(tokens, 1) - lax.axis_index("tp") * vocab), (tokens, LANES))
        g, dx, t = grad_rows(z, lse_b, lab_b, w_loc, w_tail, inv)
        d_head = grad_head(xt, g, vocab)
        d_hidden = lax.psum_scatter(dx, "tp", scatter_dimension=0, tiled=True)
        hit_sum = jnp.sum(share(jnp.sum(t.reshape(4, 8, LANES), axis=0), n, 2))
        mean_loss = ((jnp.sum(lse) - hit_sum) * inv).reshape(1)
        return mean_loss, d_hidden.astype(jnp.bfloat16), d_head

    return jax.shard_map(
        local_step,
        mesh=mesh,
        in_specs=(P(("dp", "tp"), None), P(None, "tp"), P(("dp", "tp"))),
        out_specs=(P("dp"), P(("dp", "tp"), None), P("dp", "tp")),
        check_vma=False,
    )
```

```python
import functools
import math

import jax
import jax.numpy as jnp
from jax import lax
from jax.experimental import pallas as pl
from jax.experimental.pallas import tpu as pltpu
from jax.sharding import PartitionSpec as P

MESH = pl.DeviceIdType.MESH
LANES = 128
TT = 512
CT = 512
NEG = -3.0e38
VMEM_LIMIT = 60 * 1024 * 1024


def share_kernel(n, x_ref, out_ref, send_sem, recv_sem):
    me = lax.axis_index("tp")
    barrier = pltpu.get_barrier_semaphore()

    def greet(k, carry):
        pl.semaphore_signal(barrier, inc=1, device_id={"tp": lax.rem(me + k, n)}, device_id_type=MESH)
        return carry

    lax.fori_loop(1, n, greet, 0)
    pl.semaphore_wait(barrier, n - 1)

    def copy_to(k):
        peer = lax.rem(me + k, n)
        return pltpu.make_async_remote_copy(
            src_ref=x_ref,
            dst_ref=out_ref.at[me],
            send_sem=send_sem.at[peer],
            recv_sem=recv_sem.at[me],
            device_id={"tp": peer},
            device_id_type=MESH,
        )

    def start(k, carry):
        copy_to(k).start()
        return carry

    lax.fori_loop(1, n, start, 0)
    out_ref[me] = x_ref[...]

    def finish(k, carry):
        peer = lax.rem(me + k, n)
        copy_to(k).wait_send()
        pltpu.make_async_remote_copy(
            src_ref=x_ref,
            dst_ref=out_ref.at[peer],
            send_sem=send_sem.at[peer],
            recv_sem=recv_sem.at[peer],
            device_id={"tp": peer},
            device_id_type=MESH,
        ).wait_recv()
        return carry

    lax.fori_loop(1, n, finish, 0)


def share(x, n, ident):
    return pl.pallas_call(
        functools.partial(share_kernel, n),
        name=f"share{ident}",
        out_shape=jax.ShapeDtypeStruct((n, *x.shape), x.dtype),
        in_specs=[pl.BlockSpec(memory_space=pltpu.VMEM)],
        out_specs=pl.BlockSpec(memory_space=pltpu.VMEM),
        scratch_shapes=[pltpu.SemaphoreType.DMA((n,)), pltpu.SemaphoreType.DMA((n,))],
        compiler_params=pltpu.CompilerParams(collective_id=ident, has_side_effects=True),
    )(x)


def combine_kernel(n, stat_ref, mine_ref, out_ref, got, row, send_a, recv_a, send_b, recv_b):
    me = lax.axis_index("tp")
    barrier = pltpu.get_barrier_semaphore()

    def each(body):
        def step(k, carry):
            body(lax.rem(me + k, n))
            return carry

        lax.fori_loop(1, n, step, 0)

    each(lambda peer: pl.semaphore_signal(barrier, inc=1, device_id={"tp": peer}, device_id_type=MESH))
    pl.semaphore_wait(barrier, n - 1)

    def copy(src, dst, send, recv, peer):
        return pltpu.make_async_remote_copy(
            src_ref=src, dst_ref=dst, send_sem=send, recv_sem=recv, device_id={"tp": peer}, device_id_type=MESH
        )

    def first(peer, slot):
        return copy(stat_ref.at[peer], got.at[slot], send_a.at[peer], recv_a.at[slot], peer)

    def second(peer, slot):
        return copy(row, out_ref.at[slot], send_b.at[peer], recv_b.at[slot], peer)

    each(lambda peer: first(peer, me).start())
    got[me] = stat_ref[me]
    each(lambda peer: first(peer, peer).wait_recv())
    m_all = got[:, 0, :]
    top = jnp.max(m_all, axis=0, keepdims=True)
    total = jnp.sum(got[:, 1, :] * jnp.exp(m_all - top), axis=0, keepdims=True)
    lse = top + jnp.log(total)
    first_row = lax.broadcasted_iota(jnp.int32, row.shape, 0) == 0
    mixed = jnp.where(first_row, jnp.broadcast_to(lse, row.shape), mine_ref[...])
    row[...] = mixed
    out_ref[me] = mixed
    each(lambda peer: second(peer, me).start())
    each(lambda peer: first(peer, me).wait_send())
    each(lambda peer: second(peer, peer).wait_recv())
    each(lambda peer: second(peer, me).wait_send())


def combine(stat, mine, n, ident):
    vmem = pl.BlockSpec(memory_space=pltpu.VMEM)
    return pl.pallas_call(
        functools.partial(combine_kernel, n),
        name="combine",
        out_shape=jax.ShapeDtypeStruct(stat.shape, stat.dtype),
        in_specs=[vmem, vmem],
        out_specs=vmem,
        scratch_shapes=[pltpu.VMEM(stat.shape, stat.dtype), pltpu.VMEM(mine.shape, mine.dtype)]
        + [pltpu.SemaphoreType.DMA((n,))] * 4,
        compiler_params=pltpu.CompilerParams(collective_id=ident, has_side_effects=True),
    )(stat, mine)


ORDER = [(0, 0), (1, 0), (3, 0), (0, 1), (0, 3), (2, 0), (0, 2), (1, 1)]
ORDER += [(1, 3), (3, 1), (3, 3), (2, 1), (2, 3), (1, 2), (3, 2), (2, 2)]
PLACE = {at: k for k, at in enumerate(ORDER)}
WT = 256


def fwd_kernel(n, x_ref, wt_hbm, z_ref, xt_ref, m_ref, s_ref, w_scr, x_all, stage, zb0, zb1, wsem, send, recv, pair_send, pair_recv):
    side = math.isqrt(n // 2)
    vocab, hidden = wt_hbm.shape
    padded = w_scr.shape[1]
    rows = x_ref.shape[0]
    half = rows // 2
    tiles = padded // CT
    depth = hidden // tiles
    step = pl.program_id(0)
    me = lax.axis_index("tp")
    core = lax.rem(me, 2)
    chip = me // 2
    x, y = lax.rem(chip, side), chip // side
    p, q = x + core * (y - x), y + core * (x - y)

    def device(dp, dq):
        pp, qq = lax.rem(p + dp, side), lax.rem(q + dq, side)
        return ((qq + core * (pp - qq)) * side + pp + core * (qq - pp)) * 2 + core

    def place(dp, dq):
        dp, dq = dp % side, dq % side
        a, b = PLACE[dp, dq], PLACE[dq, dp]
        return a + core * (b - a)

    def view(dp, dq, lo, count):
        return x_all.at[pl.ds(pl.multiple_of((place(dp, dq) * 2 + core) * rows + lo, half), count), :]

    def slot(dp, dq, lo):
        return ((dp % side) * side + dq % side) * 2 + (1 if lo else 0)

    sent = []

    def ici(number, dp, dq, axis, sign, lo, count):
        to = (sign, 0) if axis == "p" else (0, sign)
        rp, rq = dp - to[0], dq - to[1]
        src = x_ref if (dp, dq) == (0, 0) else view(dp, dq, lo, count)
        return pltpu.make_async_remote_copy(
            src_ref=src,
            dst_ref=view(rp, rq, lo, count),
            send_sem=send.at[number],
            recv_sem=recv.at[slot(rp, rq, lo)],
            device_id={"tp": device(to[0] % side, to[1] % side)},
            device_id_type=MESH,
        )

    def put(*args):
        ici(len(sent), *args).start()
        sent.append(args)

    def got(dp, dq, lo, count):
        v = view(dp, dq, lo, count)
        pltpu.make_async_remote_copy(
            src_ref=v, dst_ref=v, send_sem=send.at[0], recv_sem=recv.at[slot(dp, dq, lo)],
            device_id={"tp": me}, device_id_type=MESH,
        ).wait_recv()

    pair_sent = []

    def pair_copy(dp, dq):
        v = view(dp, dq, 0, rows)
        at = place(dp, dq)
        return pltpu.make_async_remote_copy(
            src_ref=x_ref if (dp, dq) == (0, 0) else v, dst_ref=v, send_sem=pair_send.at[at], recv_sem=pair_recv.at[at],
            device_id={"tp": me + 1 - 2 * core}, device_id_type=MESH,
        )

    def pair(dp, dq):
        pair_copy(dp, dq).start()
        pair_sent.append((dp, dq))

    def pair_got(at):
        v = x_all.at[pl.ds(pl.multiple_of((at * 2 + 1 - core) * rows, half), rows), :]
        pltpu.make_async_remote_copy(
            src_ref=v, dst_ref=v, send_sem=pair_send.at[at], recv_sem=pair_recv.at[at],
            device_id={"tp": me + 1 - 2 * core}, device_id_type=MESH,
        ).wait_recv()

    def near_q(dp):
        got(dp, -1, 0, rows)
        put(dp, -1, "q", 1, 0, half)
        got(dp, 1, 0, rows)
        put(dp, 1, "q", -1, half, half)
        pair(dp, -1)
        pair(dp, 1)

    def far_q(dp):
        got(dp, 2, 0, half)
        got(dp, 2, half, half)
        pair(dp, 2)

    def both_q(dp):
        put(dp, 0, "q", 1, 0, rows)
        put(dp, 0, "q", -1, 0, rows)

    def head_copy(t, count):
        return pltpu.make_async_copy(
            wt_hbm.at[pl.ds(pl.multiple_of(t * WT, WT), count), :],
            stage.at[lax.rem(t, 2), pl.ds(0, count), :],
            wsem.at[lax.rem(t, 2)],
        )

    whole = vocab // WT
    rest = vocab - whole * WT

    def turn(lo, hi):
        def body(t, carry):
            head_copy(t, WT).wait()
            w_scr[:, pl.ds(pl.multiple_of(t * WT, WT), WT)] = stage[lax.rem(t, 2)].T

            @pl.when(t + 2 < whole)
            def _():
                head_copy(t + 2, WT).start()

            @pl.when(t + 2 == whole)
            def _():
                head_copy(whole, rest).start()

            return carry

        lax.fori_loop(lo, hi, body, 0)

    def services(k):
        if k == 0:
            barrier = pltpu.get_barrier_semaphore()
            for peer in (device(1, 0), device(side - 1, 0), device(0, 1), device(0, side - 1), me + 1 - 2 * core):
                pl.semaphore_signal(barrier, inc=1, device_id={"tp": peer}, device_id_type=MESH)
            head_copy(0, WT).start()
            head_copy(1, WT).start()
            pl.semaphore_wait(barrier, 5)
            put(0, 0, "p", 1, 0, rows)
            put(0, 0, "p", -1, 0, rows)
            pair(0, 0)
            both_q(0)
            x_all[pl.ds(pl.multiple_of(core * rows, rows), rows), :] = x_ref[...]
            turn(0, whole // 3)
            got(-1, 0, 0, rows)
            put(-1, 0, "p", 1, 0, half)
            got(1, 0, 0, rows)
            put(1, 0, "p", -1, half, half)
            pair(-1, 0)
            pair(1, 0)
            both_q(1)
            both_q(-1)
            turn(whole // 3, 2 * whole // 3)
            got(2, 0, 0, half)
            got(2, 0, half, half)
            pair(2, 0)
            both_q(2)
            near_q(0)
            turn(2 * whole // 3, whole)
            stage[whole % 2, pl.ds(rest, WT - rest), :] = jnp.zeros((WT - rest, hidden), jnp.bfloat16)
            head_copy(whole, rest).wait()
            w_scr[:, pl.ds(whole * WT, WT)] = stage[whole % 2].T
        if k == 1:
            near_q(1)
            far_q(0)
        if k == 2:
            near_q(-1)
            far_q(1)
        if k == 3:
            near_q(2)
            far_q(-1)
        if k == 4:
            far_q(2)
        pair_got(2 * k)
        pair_got(2 * k + 1)

    @pl.when(step == 0)
    def _():
        services(0)

    m_ref[...] = jnp.full(m_ref.shape, NEG, jnp.float32)
    s_ref[...] = jnp.zeros(s_ref.shape, jnp.float32)
    lane = lax.broadcasted_iota(jnp.int32, (32, LANES), 1)
    here = pl.ds(pl.multiple_of(step * TT, TT), TT)

    def product(j, zb):
        zb[...] = jnp.dot(
            x_all[here, :], w_scr[:, pl.ds(pl.multiple_of(j * CT, CT), CT)], preferred_element_type=jnp.float32
        )
        at = pl.ds(pl.multiple_of(j * depth, depth), depth)
        xt_ref[at, :] = x_all[here, at].T

    def absorb(j, zb):
        last = CT // LANES - 1
        room = vocab - j * CT - last * LANES
        for r in range(0, TT, 32):
            part = pl.ds(r, 32)
            zs = [zb[part, pl.ds(k * LANES, LANES)] for k in range(CT // LANES)]
            for k in range(CT // LANES):
                z_ref[part, pl.ds(pl.multiple_of(j * CT + k * LANES, LANES), LANES)] = zs[k]
            zs[last] = jnp.where(lane < room, zs[last], NEG)
            m_old = m_ref[part, :]
            m_new = m_old
            for z in zs:
                m_new = jnp.maximum(m_new, z)
            total = s_ref[part, :] * jnp.exp(m_old - m_new)
            for z in zs:
                total = total + jnp.exp(z - m_new)
            m_ref[part, :] = m_new
            s_ref[part, :] = total

    product(0, zb0)

    def two(k, carry):
        product(2 * k + 1, zb1)
        absorb(2 * k, zb0)
        product(2 * k + 2, zb0)
        absorb(2 * k + 1, zb1)
        return carry

    lax.fori_loop(0, tiles // 2 - 1, two, 0)
    for k in range(1, len(ORDER) // 2):

        @pl.when(step == k - 1)
        def _(k=k):
            services(k)

    product(tiles - 1, zb1)
    absorb(tiles - 2, zb0)
    absorb(tiles - 1, zb1)

    @pl.when(step == pl.num_programs(0) - 1)
    def _():
        for number, args in enumerate(sent):
            ici(number, *args).wait_send()
        for args in pair_sent:
            pair_copy(*args).wait_send()


def forward(x, wt, n, ident):
    rows, hidden = x.shape
    tokens = rows * n
    padded = wt.shape[0] // LANES * LANES + LANES
    copies = 2 + 2 + 2 * 4 + 2 * 4
    return pl.pallas_call(
        functools.partial(fwd_kernel, n),
        name="forward",
        grid=(tokens // TT,),
        out_shape=(
            jax.ShapeDtypeStruct((tokens, padded), jnp.float32),
            jax.ShapeDtypeStruct((hidden, tokens), jnp.bfloat16),
            jax.ShapeDtypeStruct((tokens, LANES), jnp.float32),
            jax.ShapeDtypeStruct((tokens, LANES), jnp.float32),
        ),
        in_specs=[
            pl.BlockSpec((rows, hidden), lambda i: (0, 0), pipeline_mode=pl.Buffered(1)),
            pl.BlockSpec(memory_space=pl.ANY),
        ],
        out_specs=(
            pl.BlockSpec((TT, padded), lambda i: (i, 0)),
            pl.BlockSpec((hidden, TT), lambda i: (0, i)),
            pl.BlockSpec((TT, LANES), lambda i: (i, 0)),
            pl.BlockSpec((TT, LANES), lambda i: (i, 0)),
        ),
        scratch_shapes=[
            pltpu.VMEM((hidden, padded), jnp.bfloat16),
            pltpu.VMEM((tokens, hidden), jnp.bfloat16),
            pltpu.VMEM((2, WT, hidden), jnp.bfloat16),
            pltpu.VMEM((TT, CT), jnp.float32),
            pltpu.VMEM((TT, CT), jnp.float32),
            pltpu.SemaphoreType.DMA((2,)),
            pltpu.SemaphoreType.DMA((copies,)),
            pltpu.SemaphoreType.DMA((n,)),
            pltpu.SemaphoreType.DMA((n // 2,)),
            pltpu.SemaphoreType.DMA((n // 2,)),
        ],
        compiler_params=pltpu.CompilerParams(
            vmem_limit_bytes=67_043_328, collective_id=ident, has_side_effects=True
        ),
        cost_estimate=pl.CostEstimate(flops=2 * tokens * hidden * padded, bytes_accessed=6 * tokens * padded, transcendentals=0),
    )(x, wt)


def grad_kernel(inv, chips_ref, z_ref, lse_ref, lab_ref, wt_hbm, g_ref, dx_hbm, t_ref, w_scr, g0, g1, dx0, dx1, sem, out_sem):
    padded, hidden = w_scr.shape
    vocab = wt_hbm.shape[0]
    step = pl.program_id(0)
    steps = pl.num_programs(0)
    pieces = padded // CT
    width = hidden // pieces
    lane = lax.broadcasted_iota(jnp.int32, (32, LANES), 1)

    def probs(j, g):
        for r in range(0, TT, 32):
            rows = pl.ds(r, 32)
            lse = lse_ref[rows, :]
            rel = lab_ref[rows, :] - j * CT
            t = t_ref[...]
            for k in range(CT // LANES):
                at = pl.ds(pl.multiple_of(j * CT + k * LANES, LANES), LANES)
                z = z_ref[rows, at]
                p = jnp.exp(z - lse)
                hit = rel == lane + k * LANES
                t = t + jnp.where(hit, z, 0.0)
                gv = jnp.where(hit, p - inv, p).astype(jnp.bfloat16)
                g[rows, at] = gv
                g_ref[rows, at] = gv
            t_ref[...] = t

    @pl.when(step == 0)
    def _():
        load = pltpu.make_async_copy(wt_hbm, w_scr.at[pl.ds(0, vocab), :], sem)
        load.start()
        w_scr[pl.ds(vocab, padded - vocab), :] = jnp.zeros((padded - vocab, hidden), jnp.bfloat16)
        t_ref[...] = jnp.zeros(t_ref.shape, jnp.float32)

        def piece(j, carry):
            probs(j, g0)
            return carry

        lax.fori_loop(0, pieces, piece, 0)
        load.wait()

    per_chip = TT // 2

    def leave(at, dx):
        return [
            pltpu.make_async_copy(
                dx.at[pl.ds(k * per_chip, per_chip), :],
                dx_hbm.at[pl.ds(pl.multiple_of(chips_ref[at * 2 + k] * per_chip, per_chip), per_chip), :],
                out_sem.at[lax.rem(at, 2), k],
            )
            for k in range(2)
        ]

    def back(j, g, dx):
        at = pl.ds(pl.multiple_of(j * width, width), width)
        dx[:, at] = jnp.dot(g[...], w_scr[:, at], preferred_element_type=jnp.float32)

    for parity, (now, later, dx) in enumerate(((g1, g0, dx1), (g0, g1, dx0))):

        @pl.when((step > 2) & (lax.rem(step, 2) == parity))
        def _(dx=dx):
            for c in leave(step - 3, dx):
                c.wait()

        @pl.when((step > 0) & (step < steps - 1) & (lax.rem(step, 2) == parity))
        def _(now=now, later=later, dx=dx):
            def piece(j, carry):
                back(j, now, dx)
                probs(j, later)
                return carry

            lax.fori_loop(0, pieces, piece, 0)

        if parity == 0:

            @pl.when(step == steps - 1)
            def _(now=now, dx=dx):
                def piece(j, carry):
                    back(j, now, dx)
                    return carry

                lax.fori_loop(0, pieces, piece, 0)

        @pl.when((step > 0) & (lax.rem(step, 2) == parity))
        def _(dx=dx):
            for c in leave(step - 1, dx):
                c.start()

    @pl.when(step == steps - 1)
    def _():
        for c in leave(step - 2, dx0) + leave(step - 1, dx1):
            c.wait()


def grad_rows(chips, z, lse, lab, wt, inv):
    tokens, padded = z.shape
    hidden = wt.shape[1]
    steps = tokens // TT
    ahead = lambda i: (jnp.minimum(i, steps - 1), 0)
    return pl.pallas_call(
        functools.partial(grad_kernel, inv),
        name="grad_rows",
        grid=(steps + 1,),
        out_shape=(
            jax.ShapeDtypeStruct((tokens, padded), jnp.bfloat16),
            jax.ShapeDtypeStruct((tokens, hidden), jnp.float32),
            jax.ShapeDtypeStruct((32, LANES), jnp.float32),
        ),
        in_specs=[
            pl.BlockSpec(memory_space=pltpu.SMEM),
            pl.BlockSpec((TT, padded), ahead),
            pl.BlockSpec((TT, LANES), ahead),
            pl.BlockSpec((TT, LANES), ahead),
            pl.BlockSpec(memory_space=pl.ANY),
        ],
        out_specs=(
            pl.BlockSpec((TT, padded), ahead),
            pl.BlockSpec(memory_space=pl.ANY),
            pl.BlockSpec((32, LANES), lambda i: (0, 0)),
        ),
        scratch_shapes=[
            pltpu.VMEM((padded, hidden), jnp.bfloat16),
            pltpu.VMEM((TT, padded), jnp.bfloat16),
            pltpu.VMEM((TT, padded), jnp.bfloat16),
            pltpu.VMEM((TT, hidden), jnp.float32),
            pltpu.VMEM((TT, hidden), jnp.float32),
            pltpu.SemaphoreType.DMA,
            pltpu.SemaphoreType.DMA((2, 2)),
        ],
        compiler_params=pltpu.CompilerParams(vmem_limit_bytes=VMEM_LIMIT),
        cost_estimate=pl.CostEstimate(flops=2 * tokens * hidden * padded, bytes_accessed=6 * tokens * padded, transcendentals=0),
    )(chips, z, lse, lab, wt)


def head_kernel(parts, *refs):
    xts, gs, out_ref = refs[:parts], refs[parts : 2 * parts], refs[2 * parts]

    def piece(j, carry):
        rows = pl.ds(pl.multiple_of(j * TT, TT), TT)
        total = None
        for xt, g in zip(xts, gs):
            term = jnp.dot(xt[rows, :], g[...], preferred_element_type=jnp.float32)
            total = term if total is None else total + term
        out_ref[:, rows] = total.astype(jnp.bfloat16).T
        return carry

    lax.fori_loop(0, out_ref.shape[1] // TT, piece, 0)


def grad_head(xts, gs, vocab):
    hidden = xts[0].shape[0]
    tokens = sum(x.shape[1] for x in xts)
    padded = gs[0].shape[1]
    width = 256
    return pl.pallas_call(
        functools.partial(head_kernel, len(xts)),
        name="grad_head",
        grid=(padded // width,),
        out_shape=jax.ShapeDtypeStruct((vocab, hidden), jnp.bfloat16),
        in_specs=[pl.BlockSpec(x.shape, lambda i: (0, 0), pipeline_mode=pl.Buffered(1)) for x in xts]
        + [pl.BlockSpec((g.shape[0], width), lambda i: (0, i)) for g in gs],
        out_specs=pl.BlockSpec((width, hidden), lambda i: (i, 0)),
        compiler_params=pltpu.CompilerParams(vmem_limit_bytes=VMEM_LIMIT),
        cost_estimate=pl.CostEstimate(flops=2 * tokens * hidden * padded, bytes_accessed=4 * tokens * padded, transcendentals=0),
    )(*xts, *gs)


def solution(mesh):
    n = mesh.shape["tp"]

    def local_step(hid_loc, w_loc, lab_loc):
        rows, hidden = hid_loc.shape
        vocab = w_loc.shape[1]
        tokens = rows * n
        inv = 1.0 / tokens
        wt = w_loc.T
        side = math.isqrt(n // 2)
        me = lax.axis_index("tp")
        x, y = me // 2 % side, me // 2 // side
        order = jnp.array(ORDER, jnp.int32)
        chips = (y + order[:, 1]) % side * side + (x + order[:, 0]) % side
        table = jnp.array([[PLACE[a, b] for b in range(side)] for a in range(side)], jnp.int32)
        every = jnp.arange(side * side, dtype=jnp.int32)
        places = table[(every % side - x) % side, (every // side - y) % side]
        z, xt, m_lane, s_lane = forward(hid_loc, wt, n, 0)
        m_loc = jnp.max(m_lane, axis=1)
        s_loc = jnp.sum(s_lane * jnp.exp(m_lane - m_loc[:, None]), axis=1)
        local = jnp.stack([m_loc.reshape(-1, 2, rows), s_loc.reshape(-1, 2, rows)], axis=2)
        stat = jnp.pad(jnp.take(local, places, axis=0).reshape(n, 2, rows), ((0, 0), (0, 6), (0, 0)))
        mine = jnp.broadcast_to(lab_loc.astype(jnp.float32).reshape(1, rows), (8, rows))
        both = combine(stat, mine, n, 1)
        lse = both[:, 0]
        lab_rel = both[:, 1].astype(jnp.int32) - me * vocab
        in_order = lambda a: jnp.take(a.reshape(n // 2, -1), chips, axis=0).reshape(tokens, 1)
        lse_b = jnp.broadcast_to(in_order(lse + math.log(tokens)), (tokens, LANES))
        lab_b = jnp.broadcast_to(in_order(lab_rel), (tokens, LANES))
        g, dx, t = grad_rows(chips, z, lse_b, lab_b, wt, inv)
        d_hidden = lax.psum_scatter(dx, "tp", scatter_dimension=0, tiled=True)
        d_head = grad_head([xt], [g], vocab).T
        hit_sum = jnp.sum(share(jnp.sum(t.reshape(4, 8, LANES), axis=0), n, 2))
        mean_loss = ((jnp.sum(lse) - hit_sum) * inv).reshape(1)
        return mean_loss, d_hidden.astype(jnp.bfloat16), d_head

    return jax.shard_map(
        local_step,
        mesh=mesh,
        in_specs=(P(("dp", "tp"), None), P(None, "tp"), P(("dp", "tp"))),
        out_specs=(P("dp"), P(("dp", "tp"), None), P("dp", "tp")),
        check_vma=False,
    )
```

```python
import functools
import math

import jax
import jax.numpy as jnp
from jax import lax
from jax.experimental import pallas as pl
from jax.experimental.pallas import tpu as pltpu
from jax.sharding import PartitionSpec as P

MESH = pl.DeviceIdType.MESH
LANES = 128
TT = 512
CT = 512
NEG = -3.0e38
VMEM_LIMIT = 60 * 1024 * 1024


def combine_kernel(n, stat_ref, mine_ref, out_ref, got, row, send_a, recv_a, send_b, recv_b):
    me = lax.axis_index("tp")
    barrier = pltpu.get_barrier_semaphore()

    def each(body):
        def step(k, carry):
            body(lax.rem(me + k, n))
            return carry

        lax.fori_loop(1, n, step, 0)

    each(lambda peer: pl.semaphore_signal(barrier, inc=1, device_id={"tp": peer}, device_id_type=MESH))
    pl.semaphore_wait(barrier, n - 1)

    def copy(src, dst, send, recv, peer):
        return pltpu.make_async_remote_copy(
            src_ref=src, dst_ref=dst, send_sem=send, recv_sem=recv, device_id={"tp": peer}, device_id_type=MESH
        )

    def first(peer, slot):
        return copy(stat_ref.at[peer], got.at[slot], send_a.at[peer], recv_a.at[slot], peer)

    def second(peer, slot):
        return copy(row, out_ref.at[slot], send_b.at[peer], recv_b.at[slot], peer)

    each(lambda peer: first(peer, me).start())
    got[me] = stat_ref[me]
    each(lambda peer: first(peer, peer).wait_recv())
    m_all = got[:, 0, :]
    top = jnp.max(m_all, axis=0, keepdims=True)
    total = jnp.sum(got[:, 1, :] * jnp.exp(m_all - top), axis=0, keepdims=True)
    lse = top + jnp.log(total)
    first_row = lax.broadcasted_iota(jnp.int32, row.shape, 0) == 0
    mixed = jnp.where(first_row, jnp.broadcast_to(lse, row.shape), mine_ref[...])
    row[...] = mixed
    out_ref[me] = mixed
    each(lambda peer: second(peer, me).start())
    each(lambda peer: first(peer, me).wait_send())
    each(lambda peer: second(peer, peer).wait_recv())
    each(lambda peer: second(peer, me).wait_send())


def combine(stat, mine, n, ident):
    vmem = pl.BlockSpec(memory_space=pltpu.VMEM)
    return pl.pallas_call(
        functools.partial(combine_kernel, n),
        name="combine",
        out_shape=jax.ShapeDtypeStruct(stat.shape, stat.dtype),
        in_specs=[vmem, vmem],
        out_specs=vmem,
        scratch_shapes=[pltpu.VMEM(stat.shape, stat.dtype), pltpu.VMEM(mine.shape, mine.dtype)]
        + [pltpu.SemaphoreType.DMA((n,))] * 4,
        compiler_params=pltpu.CompilerParams(collective_id=ident, has_side_effects=True),
    )(stat, mine)


ORDER = [(0, 0), (1, 0), (3, 0), (0, 1), (0, 3), (2, 0), (0, 2), (1, 1)]
ORDER += [(1, 3), (3, 1), (3, 3), (2, 1), (2, 3), (1, 2), (3, 2), (2, 2)]
PLACE = {at: k for k, at in enumerate(ORDER)}
WT = 256


def fwd_kernel(n, x_ref, wt_hbm, z_ref, xt_ref, m_ref, s_ref, w_scr, x_all, stage, zb0, zb1, wsem, send, recv, pair_send, pair_recv):
    side = math.isqrt(n // 2)
    vocab, hidden = wt_hbm.shape
    padded = w_scr.shape[1]
    rows = x_ref.shape[0]
    half = rows // 2
    tiles = padded // CT
    depth = hidden // tiles
    step = pl.program_id(0)
    me = lax.axis_index("tp")
    core = lax.rem(me, 2)
    chip = me // 2
    x, y = lax.rem(chip, side), chip // side
    p, q = x + core * (y - x), y + core * (x - y)

    def device(dp, dq):
        pp, qq = lax.rem(p + dp, side), lax.rem(q + dq, side)
        return ((qq + core * (pp - qq)) * side + pp + core * (qq - pp)) * 2 + core

    def place(dp, dq):
        dp, dq = dp % side, dq % side
        a, b = PLACE[dp, dq], PLACE[dq, dp]
        return a + core * (b - a)

    def view(dp, dq, lo, count):
        return x_all.at[pl.ds(pl.multiple_of((place(dp, dq) * 2 + core) * rows + lo, half), count), :]

    def slot(dp, dq, lo):
        return ((dp % side) * side + dq % side) * 2 + (1 if lo else 0)

    sent = []

    def ici(number, dp, dq, axis, sign, lo, count):
        to = (sign, 0) if axis == "p" else (0, sign)
        rp, rq = dp - to[0], dq - to[1]
        src = x_ref if (dp, dq) == (0, 0) else view(dp, dq, lo, count)
        return pltpu.make_async_remote_copy(
            src_ref=src,
            dst_ref=view(rp, rq, lo, count),
            send_sem=send.at[number],
            recv_sem=recv.at[slot(rp, rq, lo)],
            device_id={"tp": device(to[0] % side, to[1] % side)},
            device_id_type=MESH,
        )

    def put(*args):
        ici(len(sent), *args).start()
        sent.append(args)

    def got(dp, dq, lo, count):
        v = view(dp, dq, lo, count)
        pltpu.make_async_remote_copy(
            src_ref=v, dst_ref=v, send_sem=send.at[0], recv_sem=recv.at[slot(dp, dq, lo)],
            device_id={"tp": me}, device_id_type=MESH,
        ).wait_recv()

    pair_sent = []

    def pair_copy(dp, dq):
        v = view(dp, dq, 0, rows)
        at = place(dp, dq)
        return pltpu.make_async_remote_copy(
            src_ref=x_ref if (dp, dq) == (0, 0) else v, dst_ref=v, send_sem=pair_send.at[at], recv_sem=pair_recv.at[at],
            device_id={"tp": me + 1 - 2 * core}, device_id_type=MESH,
        )

    def pair(dp, dq):
        pair_copy(dp, dq).start()
        pair_sent.append((dp, dq))

    def pair_got(at):
        v = x_all.at[pl.ds(pl.multiple_of((at * 2 + 1 - core) * rows, half), rows), :]
        pltpu.make_async_remote_copy(
            src_ref=v, dst_ref=v, send_sem=pair_send.at[at], recv_sem=pair_recv.at[at],
            device_id={"tp": me + 1 - 2 * core}, device_id_type=MESH,
        ).wait_recv()

    def near_q(dp):
        got(dp, -1, 0, rows)
        put(dp, -1, "q", 1, 0, half)
        got(dp, 1, 0, rows)
        put(dp, 1, "q", -1, half, half)
        pair(dp, -1)
        pair(dp, 1)

    def far_q(dp):
        got(dp, 2, 0, half)
        got(dp, 2, half, half)
        pair(dp, 2)

    def both_q(dp):
        put(dp, 0, "q", 1, 0, rows)
        put(dp, 0, "q", -1, 0, rows)

    def head_copy(t, count):
        return pltpu.make_async_copy(
            wt_hbm.at[pl.ds(pl.multiple_of(t * WT, WT), count), :],
            stage.at[lax.rem(t, 2), pl.ds(0, count), :],
            wsem.at[lax.rem(t, 2)],
        )

    whole = vocab // WT
    rest = vocab - whole * WT

    def turn(lo, hi):
        def body(t, carry):
            head_copy(t, WT).wait()
            w_scr[:, pl.ds(pl.multiple_of(t * WT, WT), WT)] = stage[lax.rem(t, 2)].T

            @pl.when(t + 2 < whole)
            def _():
                head_copy(t + 2, WT).start()

            @pl.when(t + 2 == whole)
            def _():
                head_copy(whole, rest).start()

            return carry

        lax.fori_loop(lo, hi, body, 0)

    def services(k):
        if k == 0:
            barrier = pltpu.get_barrier_semaphore()
            for peer in (device(1, 0), device(side - 1, 0), device(0, 1), device(0, side - 1), me + 1 - 2 * core):
                pl.semaphore_signal(barrier, inc=1, device_id={"tp": peer}, device_id_type=MESH)
            head_copy(0, WT).start()
            head_copy(1, WT).start()
            pl.semaphore_wait(barrier, 5)
            put(0, 0, "p", 1, 0, rows)
            put(0, 0, "p", -1, 0, rows)
            pair(0, 0)
            both_q(0)
            x_all[pl.ds(pl.multiple_of(core * rows, rows), rows), :] = x_ref[...]
            turn(0, whole // 3)
            got(-1, 0, 0, rows)
            put(-1, 0, "p", 1, 0, half)
            got(1, 0, 0, rows)
            put(1, 0, "p", -1, half, half)
            pair(-1, 0)
            pair(1, 0)
            both_q(1)
            both_q(-1)
            turn(whole // 3, 2 * whole // 3)
            got(2, 0, 0, half)
            got(2, 0, half, half)
            pair(2, 0)
            both_q(2)
            near_q(0)
            turn(2 * whole // 3, whole)
            stage[whole % 2, pl.ds(rest, WT - rest), :] = jnp.zeros((WT - rest, hidden), jnp.bfloat16)
            head_copy(whole, rest).wait()
            w_scr[:, pl.ds(whole * WT, WT)] = stage[whole % 2].T
        if k == 1:
            near_q(1)
            far_q(0)
        if k == 2:
            near_q(-1)
            far_q(1)
        if k == 3:
            near_q(2)
            far_q(-1)
        if k == 4:
            far_q(2)
        pair_got(2 * k)
        pair_got(2 * k + 1)

    @pl.when(step == 0)
    def _():
        services(0)

    m_ref[...] = jnp.full(m_ref.shape, NEG, jnp.float32)
    s_ref[...] = jnp.zeros(s_ref.shape, jnp.float32)
    lane = lax.broadcasted_iota(jnp.int32, (32, LANES), 1)
    here = pl.ds(pl.multiple_of(step * TT, TT), TT)

    def product(j, zb):
        zb[...] = jnp.dot(
            x_all[here, :], w_scr[:, pl.ds(pl.multiple_of(j * CT, CT), CT)], preferred_element_type=jnp.float32
        )
        at = pl.ds(pl.multiple_of(j * depth, depth), depth)
        xt_ref[at, :] = x_all[here, at].T

    def absorb(j, zb):
        last = CT // LANES - 1
        room = vocab - j * CT - last * LANES
        for r in range(0, TT, 32):
            part = pl.ds(r, 32)
            zs = [zb[part, pl.ds(k * LANES, LANES)] for k in range(CT // LANES)]
            for k in range(CT // LANES):
                z_ref[part, pl.ds(pl.multiple_of(j * CT + k * LANES, LANES), LANES)] = zs[k]
            zs[last] = jnp.where(lane < room, zs[last], NEG)
            m_old = m_ref[part, :]
            m_new = m_old
            for z in zs:
                m_new = jnp.maximum(m_new, z)
            total = s_ref[part, :] * jnp.exp(m_old - m_new)
            for z in zs:
                total = total + jnp.exp(z - m_new)
            m_ref[part, :] = m_new
            s_ref[part, :] = total

    product(0, zb0)

    def two(k, carry):
        product(2 * k + 1, zb1)
        absorb(2 * k, zb0)
        product(2 * k + 2, zb0)
        absorb(2 * k + 1, zb1)
        return carry

    lax.fori_loop(0, tiles // 2 - 1, two, 0)
    for k in range(1, len(ORDER) // 2):

        @pl.when(step == k - 1)
        def _(k=k):
            services(k)

    product(tiles - 1, zb1)
    absorb(tiles - 2, zb0)
    absorb(tiles - 1, zb1)

    @pl.when(step == pl.num_programs(0) - 1)
    def _():
        for number, args in enumerate(sent):
            ici(number, *args).wait_send()
        for args in pair_sent:
            pair_copy(*args).wait_send()


def forward(x, wt, n, ident):
    rows, hidden = x.shape
    tokens = rows * n
    padded = wt.shape[0] // LANES * LANES + LANES
    copies = 2 + 2 + 2 * 4 + 2 * 4
    return pl.pallas_call(
        functools.partial(fwd_kernel, n),
        name="forward",
        grid=(tokens // TT,),
        out_shape=(
            jax.ShapeDtypeStruct((tokens, padded), jnp.float32),
            jax.ShapeDtypeStruct((hidden, tokens), jnp.bfloat16),
            jax.ShapeDtypeStruct((tokens, LANES), jnp.float32),
            jax.ShapeDtypeStruct((tokens, LANES), jnp.float32),
        ),
        in_specs=[
            pl.BlockSpec((rows, hidden), lambda i: (0, 0), pipeline_mode=pl.Buffered(1)),
            pl.BlockSpec(memory_space=pl.ANY),
        ],
        out_specs=(
            pl.BlockSpec((TT, padded), lambda i: (i, 0)),
            pl.BlockSpec((hidden, TT), lambda i: (0, i)),
            pl.BlockSpec((TT, LANES), lambda i: (i, 0)),
            pl.BlockSpec((TT, LANES), lambda i: (i, 0)),
        ),
        scratch_shapes=[
            pltpu.VMEM((hidden, padded), jnp.bfloat16),
            pltpu.VMEM((tokens, hidden), jnp.bfloat16),
            pltpu.VMEM((2, WT, hidden), jnp.bfloat16),
            pltpu.VMEM((TT, CT), jnp.float32),
            pltpu.VMEM((TT, CT), jnp.float32),
            pltpu.SemaphoreType.DMA((2,)),
            pltpu.SemaphoreType.DMA((copies,)),
            pltpu.SemaphoreType.DMA((n,)),
            pltpu.SemaphoreType.DMA((n // 2,)),
            pltpu.SemaphoreType.DMA((n // 2,)),
        ],
        compiler_params=pltpu.CompilerParams(
            vmem_limit_bytes=67_043_328, collective_id=ident, has_side_effects=True
        ),
        cost_estimate=pl.CostEstimate(flops=2 * tokens * hidden * padded, bytes_accessed=6 * tokens * padded, transcendentals=0),
    )(x, wt)


def grad_kernel(
    n, inv, z_ref, lse_ref, lab_ref, wt_hbm, g_hbm, sum_hbm, hit_ref,
    t_ref, hits, hit_send, hit_recv, w_scr, g0, g1, dx0, dx1, pr0, pr1, sem, g_sem, out_sem, send_sem, recv_sem, free_sem,
):
    side = math.isqrt(n // 2)
    padded, hidden = w_scr.shape
    vocab = wt_hbm.shape[0]
    step = pl.program_id(0)
    steps = pl.num_programs(0)
    pieces = padded // CT
    width = hidden // pieces
    rows = TT // 4
    lane = lax.broadcasted_iota(jnp.int32, (32, LANES), 1)
    me = lax.axis_index("tp")
    core = lax.rem(me, 2)
    partner = me + 1 - 2 * core
    chip = me // 2
    x, y = lax.rem(chip, side), chip // side

    def each(body):
        def peers(k, carry):
            body(lax.rem(me + k, n))
            return carry

        lax.fori_loop(1, n, peers, 0)

    def tell(peer, slot):
        return pltpu.make_async_remote_copy(
            src_ref=t_ref.at[pl.ds(0, 8), :],
            dst_ref=hits.at[slot],
            send_sem=hit_send.at[peer],
            recv_sem=hit_recv.at[slot],
            device_id={"tp": peer},
            device_id_type=MESH,
        )

    def chip_at(place):
        dx = dy = 0
        for k, (ax, ay) in enumerate(ORDER):
            dx = dx + jnp.where(place == k, ax, 0)
            dy = dy + jnp.where(place == k, ay, 0)
        return lax.rem(y + dy, side) * side + lax.rem(x + dx, side)

    def probs(j, g):
        for r in range(0, TT, 32):
            part = pl.ds(r, 32)
            lse = lse_ref[part, :]
            rel = lab_ref[part, :] - j * CT
            t = t_ref[...]
            for k in range(CT // LANES):
                at = pl.ds(pl.multiple_of(j * CT + k * LANES, LANES), LANES)
                z = z_ref[part, at]
                p = jnp.exp(z - lse)
                hit = rel == lane + k * LANES
                t = t + jnp.where(hit, z, 0.0)
                g[part, at] = jnp.where(hit, p - inv, p).astype(jnp.bfloat16)
            t_ref[...] = t

    def g_copy(tile, par, g):
        return pltpu.make_async_copy(g, g_hbm.at[pl.ds(pl.multiple_of(tile * TT, TT), TT), :], g_sem.at[par])

    def own(dx, k):
        return dx.at[pl.ds(pl.multiple_of(2 * k * rows + core * rows, rows), rows), :]

    def trade(par, dx, pr, k):
        return pltpu.make_async_remote_copy(
            src_ref=dx.at[pl.ds(pl.multiple_of(2 * k * rows + (1 - core) * rows, rows), rows), :],
            dst_ref=pr.at[k],
            send_sem=send_sem.at[par, k],
            recv_sem=recv_sem.at[par, k],
            device_id={"tp": partner},
            device_id_type=MESH,
        )

    def leave(tile, par, dx, k):
        return pltpu.make_async_copy(own(dx, k), sum_hbm.at[chip_at(tile * 2 + k)], out_sem.at[par, k])

    def merge(tile, par, dx, pr):
        for k in range(2):
            trade(par, dx, pr, k).wait()
            at = pl.ds(pl.multiple_of(2 * k * rows + core * rows, rows), rows)
            dx[at, :] = dx[at, :] + pr[k]
            leave(tile, par, dx, k).start()

        @pl.when(tile + 2 < steps - 1)
        def _():
            pl.semaphore_signal(free_sem.at[par], inc=1, device_id={"tp": partner}, device_id_type=MESH)

    @pl.when(step == 0)
    def _():
        barrier = pltpu.get_barrier_semaphore()
        each(lambda peer: pl.semaphore_signal(barrier, inc=1, device_id={"tp": peer}, device_id_type=MESH))
        load = pltpu.make_async_copy(wt_hbm, w_scr.at[pl.ds(0, vocab), :], sem)
        load.start()
        w_scr[pl.ds(vocab, padded - vocab), :] = jnp.zeros((padded - vocab, hidden), jnp.bfloat16)
        t_ref[...] = jnp.zeros(t_ref.shape, jnp.float32)

        def piece(j, carry):
            probs(j, g0)
            return carry

        lax.fori_loop(0, pieces, piece, 0)
        g_copy(0, 0, g0).start()
        load.wait()
        pl.semaphore_wait(barrier, n - 1)

    def back(j, g, dx):
        at = pl.ds(pl.multiple_of(j * width, width), width)
        dx[:, at] = jnp.dot(g[...], w_scr[:, at], preferred_element_type=jnp.float32)

    buffers = ((dx0, pr0), (dx1, pr1))
    for parity, (now, later) in enumerate(((g1, g0), (g0, g1))):
        dx, pr = buffers[1 - parity]
        old = buffers[parity]

        def halfway(j, parity=parity, old=old):
            @pl.when((j == pieces // 2) & (step > 1))
            def _():
                merge(step - 2, parity, *old)

        @pl.when((step > 0) & (step < steps - 1) & (lax.rem(step, 2) == parity))
        def _(now=now, later=later, dx=dx, halfway=halfway):
            def piece(j, carry):
                halfway(j)
                back(j, now, dx)
                probs(j, later)
                return carry

            lax.fori_loop(0, pieces, piece, 0)

        if parity == 0:

            @pl.when(step == steps - 1)
            def _(now=now, dx=dx, halfway=halfway):
                mine = t_ref[0:8, :] + t_ref[8:16, :] + t_ref[16:24, :] + t_ref[24:32, :]
                t_ref[0:8, :] = mine
                hits[me] = mine
                each(lambda peer: tell(peer, me).start())

                def piece(j, carry):
                    halfway(j)
                    back(j, now, dx)
                    return carry

                lax.fori_loop(0, pieces, piece, 0)

        @pl.when((step > 1) & (lax.rem(step, 2) == parity))
        def _(parity=parity, old=old):
            for k in range(2):
                leave(step - 2, parity, old[0], k).wait()

        @pl.when((step > 0) & (lax.rem(step, 2) == parity))
        def _(parity=parity, now=now, dx=dx, pr=pr):
            @pl.when(step > 2)
            def _():
                pl.semaphore_wait(free_sem.at[1 - parity], 1)

            for k in range(2):
                trade(1 - parity, dx, pr, k).start()
            g_copy(step - 1, 1 - parity, now).wait()

        @pl.when((step > 0) & (step < steps - 1) & (lax.rem(step, 2) == parity))
        def _(parity=parity, later=later):
            g_copy(step, parity, later).start()

    @pl.when(step == steps - 1)
    def _():
        merge(step - 1, 1, dx1, pr1)
        each(lambda peer: tell(peer, peer).wait_recv())
        each(lambda peer: tell(peer, me).wait_send())
        hit_ref[...] = hits[...]
        for k in range(2):
            leave(step - 1, 1, dx1, k).wait()


def grad_rows(z, lse, lab, wt, n, inv, ident):
    tokens, padded = z.shape
    hidden = wt.shape[1]
    steps = tokens // TT
    ahead = lambda i: (jnp.minimum(i, steps - 1), 0)
    any_spec = pl.BlockSpec(memory_space=pl.ANY)
    return pl.pallas_call(
        functools.partial(grad_kernel, n, inv),
        name="grad_rows",
        grid=(steps + 1,),
        out_shape=(
            jax.ShapeDtypeStruct((tokens, padded), jnp.bfloat16),
            jax.ShapeDtypeStruct((n // 2, tokens // n, hidden), jnp.float32),
            jax.ShapeDtypeStruct((n, 8, LANES), jnp.float32),
        ),
        in_specs=[
            pl.BlockSpec((TT, padded), ahead),
            pl.BlockSpec((TT, LANES), ahead),
            pl.BlockSpec((TT, LANES), ahead),
            any_spec,
        ],
        out_specs=(any_spec, any_spec, pl.BlockSpec((n, 8, LANES), lambda i: (0, 0, 0))),
        scratch_shapes=[
            pltpu.VMEM((32, LANES), jnp.float32),
            pltpu.VMEM((n, 8, LANES), jnp.float32),
            pltpu.SemaphoreType.DMA((n,)),
            pltpu.SemaphoreType.DMA((n,)),
            pltpu.VMEM((padded, hidden), jnp.bfloat16),
            pltpu.VMEM((TT, padded), jnp.bfloat16),
            pltpu.VMEM((TT, padded), jnp.bfloat16),
            pltpu.VMEM((TT, hidden), jnp.float32),
            pltpu.VMEM((TT, hidden), jnp.float32),
            pltpu.VMEM((2, TT // 4, hidden), jnp.float32),
            pltpu.VMEM((2, TT // 4, hidden), jnp.float32),
            pltpu.SemaphoreType.DMA,
            pltpu.SemaphoreType.DMA((2,)),
            pltpu.SemaphoreType.DMA((2, 2)),
            pltpu.SemaphoreType.DMA((2, 2)),
            pltpu.SemaphoreType.DMA((2, 2)),
            pltpu.SemaphoreType.REGULAR((2,)),
        ],
        compiler_params=pltpu.CompilerParams(vmem_limit_bytes=67_043_328, collective_id=ident, has_side_effects=True),
        cost_estimate=pl.CostEstimate(flops=2 * tokens * hidden * padded, bytes_accessed=6 * tokens * padded, transcendentals=0),
    )(z, lse, lab, wt)


def head_kernel(parts, *refs):
    xts, gs, out_ref = refs[:parts], refs[parts : 2 * parts], refs[2 * parts]

    def piece(j, carry):
        rows = pl.ds(pl.multiple_of(j * TT, TT), TT)
        total = None
        for xt, g in zip(xts, gs):
            term = jnp.dot(xt[rows, :], g[...], preferred_element_type=jnp.float32)
            total = term if total is None else total + term
        out_ref[:, rows] = total.astype(jnp.bfloat16).T
        return carry

    lax.fori_loop(0, out_ref.shape[1] // TT, piece, 0)


def grad_head(xts, gs, vocab):
    hidden = xts[0].shape[0]
    tokens = sum(x.shape[1] for x in xts)
    padded = gs[0].shape[1]
    width = 256
    return pl.pallas_call(
        functools.partial(head_kernel, len(xts)),
        name="grad_head",
        grid=(padded // width,),
        out_shape=jax.ShapeDtypeStruct((vocab, hidden), jnp.bfloat16),
        in_specs=[pl.BlockSpec(x.shape, lambda i: (0, 0), pipeline_mode=pl.Buffered(1)) for x in xts]
        + [pl.BlockSpec((g.shape[0], width), lambda i: (0, i)) for g in gs],
        out_specs=pl.BlockSpec((width, hidden), lambda i: (i, 0)),
        compiler_params=pltpu.CompilerParams(vmem_limit_bytes=VMEM_LIMIT),
        cost_estimate=pl.CostEstimate(flops=2 * tokens * hidden * padded, bytes_accessed=4 * tokens * padded, transcendentals=0),
    )(*xts, *gs)


def solution(mesh):
    n = mesh.shape["tp"]

    def local_step(hid_loc, w_loc, lab_loc):
        rows, hidden = hid_loc.shape
        vocab = w_loc.shape[1]
        tokens = rows * n
        inv = 1.0 / tokens
        wt = w_loc.T
        side = math.isqrt(n // 2)
        me = lax.axis_index("tp")
        x, y = me // 2 % side, me // 2 // side
        order = jnp.array(ORDER, jnp.int32)
        chips = (y + order[:, 1]) % side * side + (x + order[:, 0]) % side
        table = jnp.array([[PLACE[a, b] for b in range(side)] for a in range(side)], jnp.int32)
        every = jnp.arange(side * side, dtype=jnp.int32)
        places = table[(every % side - x) % side, (every // side - y) % side]
        z, xt, m_lane, s_lane = forward(hid_loc, wt, n, 0)
        m_loc = jnp.max(m_lane, axis=1)
        s_loc = jnp.sum(s_lane * jnp.exp(m_lane - m_loc[:, None]), axis=1)
        local = jnp.stack([m_loc.reshape(-1, 2, rows), s_loc.reshape(-1, 2, rows)], axis=2)
        stat = jnp.pad(jnp.take(local, places, axis=0).reshape(n, 2, rows), ((0, 0), (0, 6), (0, 0)))
        mine = jnp.broadcast_to(lab_loc.astype(jnp.float32).reshape(1, rows), (8, rows))
        both = combine(stat, mine, n, 1)
        lse = both[:, 0]
        lab_rel = both[:, 1].astype(jnp.int32) - me * vocab
        in_order = lambda a: jnp.take(a.reshape(n // 2, -1), chips, axis=0).reshape(tokens, 1)
        lse_b = jnp.broadcast_to(in_order(lse + math.log(tokens)), (tokens, LANES))
        lab_b = jnp.broadcast_to(in_order(lab_rel), (tokens, LANES))
        g, dx, t = grad_rows(z, lse_b, lab_b, wt, n, inv, 3)
        same_core = [list(range(k, n, 2)) for k in range(2)]
        d_hidden = lax.psum_scatter(
            dx.reshape(tokens // 2, hidden), "tp", scatter_dimension=0, axis_index_groups=same_core, tiled=True
        )
        d_head = grad_head([xt], [g], vocab).T
        hit_sum = jnp.sum(t)
        mean_loss = ((jnp.sum(lse) - hit_sum) * inv).reshape(1)
        return mean_loss, d_hidden.astype(jnp.bfloat16), d_head

    return jax.shard_map(
        local_step,
        mesh=mesh,
        in_specs=(P(("dp", "tp"), None), P(None, "tp"), P(("dp", "tp"))),
        out_specs=(P("dp"), P(("dp", "tp"), None), P("dp", "tp")),
        check_vma=False,
    )
```
